256 devices in a mesh: ea: 64 (over y, x_lo, z), sa: 4 (over x_hi, core).
Axes of the slice: x: 4 (x_hi: 2, x_lo: 2; x = x_hi * 2 + x_lo), y: 4, z: 8, core: 2. Of those that a mesh axis runs over, the one named last changes fastest.
Arguments:
- lesser: bfloat16 [2, 1024, 2, 256, 256], P(None, 'ea', None, 'sa'), may hold values from -30 to 30, as said below
- greater: bfloat16 [2, 1024, 2, 256, 256], P(None, 'ea', None, 'sa'), may hold values from -30 to 30, as said below
Outputs:
- polar: float32 [2, 1024, 2, 256, 256], P(None, 'ea', None, 'sa')
- pol_norm: float32 [1], replicated
The draws below stay inside these ranges and needn't reach their ends.
Inputs may be any that keep to these rules, and one draw needn't show every extreme that they name: `lesser`: Real-valued entries, independent from energy to energy. `greater`: Real-valued entries, independent from energy to energy.
All inputs are finite; a program needn't handle non-finite values.
Results may differ from the reference program's by a relative error of at most 0.0049.
Values may be sent and summed in bfloat16 or wider, within the bound.
A program may use at most 128 MiB of HBM per device.

```python
import math
import jax
import jax.numpy as jnp
from jax import lax

NE = 1024
ORB = 256
BLOCKS = 2


def green_draw(key):
    first, second = jax.random.split(key, 2)
    shape = (2, NE, BLOCKS, ORB, ORB)
    rows = jnp.arange(ORB, dtype=jnp.float32) / ORB
    row_scale = 10.0 ** (0.5 * rows - 0.25)
    values = jax.random.truncated_normal(first, -4.0, 4.0, shape, jnp.float32)
    column_scale = 10.0 ** (jax.random.uniform(second, (1, 1, BLOCKS, 1, ORB), jnp.float32) - 0.5)
    return values * row_scale[None, None, None, :, None] * column_scale


def draw_lesser(key, part):
    return green_draw(jax.random.fold_in(key, 11)).astype(jnp.bfloat16)


def draw_greater(key, part):
    return green_draw(jax.random.fold_in(key, 23)).astype(jnp.bfloat16)


def setup_inputs(seed: int = 0) -> dict:
    keys = jax.random.split(jax.random.key(seed), 3)
    return {
        "lesser": draw_lesser(jax.random.fold_in(keys[2], 71), 0),
        "greater": draw_greater(jax.random.fold_in(keys[2], 71), 0),
    }


def energy_tables(count):
    index = jnp.arange(count, dtype=jnp.int32)
    phase = index[:, None] * index[None, :] % count
    angle = phase.astype(jnp.float32) * (2.0 * math.pi / count)
    return (jnp.cos(angle).astype(jnp.bfloat16), jnp.sin(angle).astype(jnp.bfloat16))

def spectra(columns, cosine, sine):
    stacked = jnp.concatenate(columns, axis=1)
    return (jnp.dot(cosine, stacked, preferred_element_type=jnp.float32), jnp.dot(sine, stacked, preferred_element_type=jnp.float32))

def split_spectrum(cos_part, sin_part, which, width):
    real_cols = slice(2 * which * width, (2 * which + 1) * width)
    imag_cols = slice((2 * which + 1) * width, (2 * which + 2) * width)
    spec_re = cos_part[:, real_cols] + sin_part[:, imag_cols]
    spec_im = cos_part[:, imag_cols] - sin_part[:, real_cols]
    return (spec_re, spec_im)

def polarize(less_re, less_im, great_re, great_im, cosine, sine, count):
    width = less_re.shape[1]
    prod_re = (less_re * great_re + less_im * great_im).astype(jnp.bfloat16)
    prod_im = (less_im * great_re - less_re * great_im).astype(jnp.bfloat16)
    cos_part, sin_part = spectra([prod_re, prod_im], cosine, sine)
    corr_re = cos_part[:, :width] - sin_part[:, width:]
    corr_im = cos_part[:, width:] + sin_part[:, :width]
    weight = float(count) ** (-1.5)
    return jnp.stack([weight * corr_im, -weight * corr_re])

def reference(lesser, greater):
    cosine, sine = energy_tables(NE)
    group = ORB * 16
    groups = BLOCKS * ORB * ORB // group
    less_groups = lesser.reshape(2, NE, groups, group).transpose(2, 0, 1, 3)
    great_groups = greater.reshape(2, NE, groups, group).transpose(2, 0, 1, 3)

    def one_group(pair):
        less_part, great_part = pair
        cos_part, sin_part = spectra([less_part[0], less_part[1], great_part[0], great_part[1]], cosine, sine)
        less_re, less_im = split_spectrum(cos_part, sin_part, 0, group)
        great_re, great_im = split_spectrum(cos_part, sin_part, 1, group)
        return polarize(less_re, less_im, great_re, great_im, cosine, sine, NE)
    polar_groups = lax.map(one_group, (less_groups, great_groups))
    polar = polar_groups.transpose(1, 2, 0, 3).reshape(2, NE, BLOCKS, ORB, ORB)
    total = jnp.sum(polar * polar)
    pol_norm = jnp.sqrt(total / (NE * BLOCKS * ORB * ORB) + 1e-06).reshape(1)
    return (polar, pol_norm)
```

```python
import functools
import math

import jax
import jax.numpy as jnp
from jax import lax
from jax.experimental import pallas as pl
from jax.experimental.pallas import tpu as pltpu
from jax.sharding import Mesh
from jax.sharding import PartitionSpec as P

EA = ("ea_0", "ea_1", "ea_2")
SA = ("sa_0", "sa_1")
MESH = pl.DeviceIdType.MESH
STEP = 32
F32 = jnp.float32
BF16 = jnp.bfloat16


def base_tables(count):
    energy = jnp.arange(count, dtype=jnp.int32)
    coarse = jnp.arange(count // STEP, dtype=jnp.int32) * STEP
    fine = jnp.arange(STEP, dtype=jnp.int32)
    unit = 2.0 * math.pi / count
    tables = []
    for index in (coarse, fine):
        angle = (index[:, None] * energy[None, :] % count).astype(F32) * unit
        tables += [jnp.cos(angle), jnp.sin(angle)]
    return tables


def kernel(sizes, less_ref, great_ref, cos_hi, sin_hi, cos_lo, sin_lo, out_ref, norm_ref,
           stage, shuffle, send_in, recv_in, table_a, table_b, prod, send_out, recv_out,
           square, norm_own, norm_sa, norm_ea, norm_all,
           load_sem, send_sem, recv_in_sem, recv_out_sem, norm_sem):
    ny, nx, nz, n0, n1 = sizes
    peers = ny * nx * nz
    own, blocks, count = 16, 2, 16 * peers
    columns = less_ref.shape[-1]
    y, x, z = (lax.axis_index(a) for a in EA)
    s0, s1 = (lax.axis_index(a) for a in SA)
    me = (y * nx + x) * nz + z
    me_sa = s0 * n1 + s1

    def partner(t):
        m, q = lax.rem(t, nz), t // nz
        dz = lax.rem(m, 2) * ((m + 1) // 2) + (1 - lax.rem(m, 2)) * lax.rem(nz - m // 2, nz)
        py, px, pz = lax.rem(y + q // nx, ny), lax.rem(x + lax.rem(q, nx), nx), lax.rem(z + dz, nz)
        return (py * nx + px) * nz + pz, (py, px, pz, s0, s1)

    def partner_sa(t):
        other = lax.rem(me_sa + t, n0 * n1)
        return (y, x, z, other // n1, lax.rem(other, n1))

    loads = [pltpu.make_async_copy(ref, stage.at[n], load_sem.at[n])
             for n, ref in enumerate((less_ref, great_ref))]
    for load in loads:
        load.start()

    barrier = pltpu.get_barrier_semaphore()

    @pl.loop(1, peers)
    def _(t):
        pl.semaphore_signal(barrier, inc=1, device_id=partner(t)[1], device_id_type=MESH)

    for t in range(1, n0 * n1):
        pl.semaphore_signal(barrier, inc=1, device_id=partner_sa(t), device_id_type=MESH)

    for load in loads:
        load.wait()
    tiles = peers // 16
    for which in range(2):
        for part in range(2):

            @pl.loop(0, blocks * tiles)
            def _(n, which=which, part=part):
                block, tile = n // tiles, lax.rem(n, tiles)
                rows = pl.ds(pl.multiple_of(tile * 16, 16), 16)
                for h in range(columns // 128):
                    lanes = slice(h * 128, (h + 1) * 128)
                    shuffle[h] = stage[which, part, :, block, rows, lanes].astype(F32).reshape(own * 16, 128)
                    for i in range(16):
                        send_in[block, tile * 16 + i, 2 * which + part, :, lanes] = shuffle[
                            h, pl.ds(i, own, stride=16), :].astype(BF16)

    for block in range(blocks):
        for q in range(4):
            recv_in[block, q, me] = send_in[block, me, q]

    pl.semaphore_wait(barrier, peers - 1 + n0 * n1 - 1)

    def copy_in(block, t):
        other, device = partner(t)
        return pltpu.make_async_remote_copy(
            src_ref=send_in.at[block, other], dst_ref=recv_in.at[block, :, me],
            send_sem=send_sem.at[block], recv_sem=recv_in_sem.at[block],
            device_id=device, device_id_type=MESH)

    def copy_out(block, t):
        other, device = partner(t)
        return pltpu.make_async_remote_copy(
            src_ref=send_out.at[block, other], dst_ref=recv_out.at[block, me],
            send_sem=send_sem.at[blocks + block], recv_sem=recv_out_sem.at[block],
            device_id=device, device_id_type=MESH)

    def copy_norm(t):
        return pltpu.make_async_remote_copy(
            src_ref=norm_all, dst_ref=norm_ea.at[me],
            send_sem=norm_sem.at[2], recv_sem=norm_sem.at[3],
            device_id=partner(t)[1], device_id_type=MESH)

    def copy_norm_sa(t):
        return pltpu.make_async_remote_copy(
            src_ref=norm_own, dst_ref=norm_sa.at[me_sa],
            send_sem=norm_sem.at[0], recv_sem=norm_sem.at[1],
            device_id=partner_sa(t), device_id_type=MESH)

    def all_of(ref, sem):
        return pltpu.make_async_remote_copy(
            src_ref=ref, dst_ref=ref, send_sem=sem, recv_sem=sem,
            device_id=partner(1)[1], device_id_type=MESH)

    for block in range(blocks):

        @pl.loop(1, peers)
        def _(t, block=block):
            copy_in(block, t).start()

    @pl.loop(0, count // STEP)
    def _(n):
        c_hi, s_hi = cos_hi[pl.ds(n, 1), :], sin_hi[pl.ds(n, 1), :]
        c_lo, s_lo = cos_lo[...], sin_lo[...]
        cosine = (c_hi * c_lo - s_hi * s_lo).astype(BF16)
        sine = (s_hi * c_lo + c_hi * s_lo).astype(BF16)
        rows = pl.ds(pl.multiple_of(n * STEP, STEP), STEP)
        table_a[rows, :count] = cosine
        table_a[rows, count:] = sine
        table_b[rows, :count] = -sine
        table_b[rows, count:] = cosine

    square[...] = jnp.zeros_like(square)
    strip = min(256, count)
    weight = float(count) ** (-1.5)

    def dot(a, b):
        return jnp.dot(a, b, preferred_element_type=F32)

    for block in range(blocks):
        all_of(recv_in.at[block, :, pl.ds(0, peers - 1)], recv_in_sem.at[block]).wait_recv()

        @pl.loop(0, count // strip)
        def _(n, block=block):
            rows = pl.ds(pl.multiple_of(n * strip, strip), strip)
            rows_im = pl.ds(pl.multiple_of(n * strip + count, strip), strip)
            less = recv_in[block, 0:2].reshape(2 * count, columns)
            great = recv_in[block, 2:4].reshape(2 * count, columns)
            less_re, less_im = dot(table_a[rows, :], less), dot(table_b[rows, :], less)
            great_re, great_im = dot(table_a[rows, :], great), dot(table_b[rows, :], great)
            prod[rows, :] = (less_im * great_re - less_re * great_im).astype(BF16)
            prod[rows_im, :] = (less_re * great_re + less_im * great_im).astype(BF16)

        @pl.loop(0, count // strip)
        def _(n, block=block):
            rows = pl.ds(pl.multiple_of(n * strip, strip), strip)
            polar_re = weight * dot(table_a[rows, :], prod[...])
            polar_im = -weight * dot(table_b[rows, :], prod[...])
            for part, value in enumerate((polar_re, polar_im)):
                square[...] += jnp.sum((value * value).reshape(strip // 8, 8, columns), axis=0)
                send_out[block, pl.ds(n * (strip // own), strip // own), part] = value.astype(BF16).reshape(
                    strip // own, own, columns)

        if block == blocks - 1:
            total = jnp.sum(square[...], axis=0, keepdims=True)
            norm_own[...] = functools.reduce(
                jnp.add, [total[:, n * 128:(n + 1) * 128] for n in range(columns // 128)])
            norm_sa[me_sa] = norm_own[...]
            for t in range(1, n0 * n1):
                copy_norm_sa(t).start()
            if n0 * n1 > 1:
                all_of(norm_sa.at[pl.ds(0, n0 * n1 - 1)], norm_sem.at[1]).wait_recv()
            norm_all[...] = functools.reduce(jnp.add, [norm_sa[n] for n in range(n0 * n1)])
            norm_ea[me] = norm_all[...]

            @pl.loop(1, peers)
            def _(t):
                copy_norm(t).start()

        recv_out[block, me] = send_out[block, me]

        @pl.loop(1, peers)
        def _(t, block=block):
            copy_out(block, t).start()

    for block in range(blocks):
        all_of(recv_out.at[block, pl.ds(0, peers - 1)], recv_out_sem.at[block]).wait_recv()
        for part in range(2):

            @pl.loop(0, tiles)
            def _(tile, block=block, part=part):
                rows = pl.ds(pl.multiple_of(tile * 16, 16), 16)
                for h in range(columns // 128):
                    lanes = slice(h * 128, (h + 1) * 128)
                    for i in range(16):
                        shuffle[h, pl.ds(i, own, stride=16), :] = recv_out[
                            block, tile * 16 + i, part, :, lanes].astype(F32)
                    out_ref[part, :, block, rows, lanes] = shuffle[h].reshape(own, 16, 128).astype(out_ref.dtype)

    all_of(norm_ea.at[pl.ds(0, peers - 1)], norm_sem.at[3]).wait_recv()
    norm = jnp.sum(jnp.sum(norm_ea[...], axis=0), axis=-1, keepdims=True)
    entries = count * blocks * peers * n0 * n1 * columns
    norm_ref[...] = jnp.broadcast_to(jnp.sqrt(norm / entries + 1e-06), norm_ref.shape)

    for block in range(blocks):
        all_of(recv_in.at[block, :, pl.ds(0, peers - 1)], send_sem.at[block]).wait_send()
        all_of(recv_out.at[block, pl.ds(0, peers - 1)], send_sem.at[blocks + block]).wait_send()
    if n0 * n1 > 1:
        all_of(norm_sa.at[pl.ds(0, n0 * n1 - 1)], norm_sem.at[0]).wait_send()
    all_of(norm_ea.at[pl.ds(0, peers - 1)], norm_sem.at[2]).wait_send()


def body(sizes, lesser, greater):
    ny, nx, nz, n0, n1 = sizes
    peers = ny * nx * nz
    own, blocks = 16, 2
    count = own * peers
    columns = lesser.shape[-1]
    vmem = pl.BlockSpec(memory_space=pltpu.VMEM)
    hbm = pl.BlockSpec(memory_space=pl.ANY)
    polar, norm = pl.pallas_call(
        functools.partial(kernel, sizes),
        out_shape=[jax.ShapeDtypeStruct(lesser.shape, BF16), jax.ShapeDtypeStruct((1, 128), F32)],
        in_specs=[hbm, hbm] + [vmem] * 4,
        out_specs=[vmem, vmem],
        scratch_shapes=[
            pltpu.VMEM((2,) + lesser.shape, BF16),
            pltpu.VMEM((columns // 128, own * 16, 128), F32),
            pltpu.VMEM((blocks, peers, 4, own, columns), BF16),
            pltpu.VMEM((blocks, 4, peers, own, columns), BF16),
            pltpu.VMEM((count, 2 * count), BF16),
            pltpu.VMEM((count, 2 * count), BF16),
            pltpu.VMEM((2 * count, columns), BF16),
            pltpu.VMEM((blocks, peers, 2, own, columns), BF16),
            pltpu.VMEM((blocks, peers, 2, own, columns), BF16),
            pltpu.VMEM((8, columns), F32),
            pltpu.VMEM((1, 128), F32),
            pltpu.VMEM((n0 * n1, 1, 128), F32),
            pltpu.VMEM((peers, 1, 128), F32),
            pltpu.VMEM((1, 128), F32),
            pltpu.SemaphoreType.DMA((2,)),
            pltpu.SemaphoreType.DMA((2 * blocks,)),
            pltpu.SemaphoreType.DMA((blocks,)),
            pltpu.SemaphoreType.DMA((blocks,)),
            pltpu.SemaphoreType.DMA((4,)),
        ],
        compiler_params=pltpu.CompilerParams(
            collective_id=0, has_side_effects=True, vmem_limit_bytes=60 * 1024 * 1024),
        name="polarize",
    )(lesser, greater, *base_tables(count))
    return polar.astype(F32), norm[0, :1]


def solution(mesh):
    sizes = (4, 2, 8, 2, 2)
    finer = Mesh(mesh.devices.reshape(sizes), EA + SA)
    spec = P(None, EA, None, SA, None)
    return jax.shard_map(functools.partial(body, sizes), mesh=finer, in_specs=(spec, spec),
                         out_specs=(spec, P()), check_vma=False)
```

```python
import functools
import math

import jax
import jax.numpy as jnp
from jax import lax
from jax.experimental import pallas as pl
from jax.experimental.pallas import tpu as pltpu
from jax.sharding import Mesh
from jax.sharding import PartitionSpec as P

EA = ("ea_0", "ea_1", "ea_2")
SA = ("sa_0", "sa_1")
MESH = pl.DeviceIdType.MESH
STEP = 32
F32 = jnp.float32
BF16 = jnp.bfloat16


def kernel(sizes, less_ref, great_ref, recv_out, norm_ref,
           stage, shuffle, send_in, recv_in, base, table_a, table_b, prod, send_out,
           square, norm_own, norm_sa, norm_ea, norm_all,
           load_sem, send_sem, recv_in_sem, recv_out_sem, norm_sem):
    ny, nx, nz, n0, n1 = sizes
    peers = ny * nx * nz
    own, blocks, count = 16, 2, 16 * peers
    columns = less_ref.shape[-1]
    y, x, z = (lax.axis_index(a) for a in EA)
    s0, s1 = (lax.axis_index(a) for a in SA)
    me = (y * nx + x) * nz + z
    me_sa = s0 * n1 + s1

    along_z = [(dz + 1) // 2 if dz % 2 else (nz - dz // 2) % nz for dz in range(nz)]
    pz = [lax.rem(z + dz, nz) for dz in along_z]

    def each_partner(visit):
        for dz in range(1, nz):
            visit((y * nx + x) * nz + pz[dz], (y, x, pz[dz], s0, s1))

        @pl.loop(1, ny * nx)
        def _(q):
            py, px = lax.rem(y + q // nx, ny), lax.rem(x + lax.rem(q, nx), nx)
            for dz in range(nz):
                visit((py * nx + px) * nz + pz[dz], (py, px, pz[dz], s0, s1))

    def partner_sa(t):
        other = lax.rem(me_sa + t, n0 * n1)
        return (y, x, z, other // n1, lax.rem(other, n1))

    loads = [pltpu.make_async_copy(ref, to, load_sem.at[n]) for n, (ref, to) in enumerate(
        ((less_ref, stage.at[0]), (great_ref, stage.at[1])))]
    barrier = pltpu.get_barrier_semaphore()
    each_partner(lambda other, device: pl.semaphore_signal(
        barrier, inc=1, device_id=device, device_id_type=MESH))

    for t in range(1, n0 * n1):
        pl.semaphore_signal(barrier, inc=1, device_id=partner_sa(t), device_id_type=MESH)

    for load in loads:
        load.start()

    for load in loads:
        load.wait()
    tiles = peers // 16
    for which in range(2):
        for part in range(2):

            @pl.loop(0, blocks * tiles)
            def _(n, which=which, part=part):
                block, tile = n // tiles, lax.rem(n, tiles)
                rows = pl.ds(pl.multiple_of(tile * 16, 16), 16)
                for h in range(columns // 128):
                    lanes = slice(h * 128, (h + 1) * 128)
                    shuffle[h] = stage[which, part, :, block, rows, lanes].astype(F32).reshape(own * 16, 128)
                    for i in range(16):
                        send_in[block, tile * 16 + i, 2 * which + part, :, lanes] = shuffle[
                            h, pl.ds(i, own, stride=16), :].astype(BF16)

    for block in range(blocks):
        for q in range(4):
            recv_in[block, q, me] = send_in[block, me, q]

    pl.semaphore_wait(barrier, peers - 1 + n0 * n1 - 1)

    def copy_in(block, other, device):
        return pltpu.make_async_remote_copy(
            src_ref=send_in.at[block, other], dst_ref=recv_in.at[block, :, me],
            send_sem=send_sem.at[block], recv_sem=recv_in_sem.at[block],
            device_id=device, device_id_type=MESH)

    def copy_out(block, other, device):
        return pltpu.make_async_remote_copy(
            src_ref=send_out.at[block, other], dst_ref=recv_out.at[block, me],
            send_sem=send_sem.at[blocks + block], recv_sem=recv_out_sem.at[block],
            device_id=device, device_id_type=MESH)

    def copy_norm(other, device):
        return pltpu.make_async_remote_copy(
            src_ref=norm_all, dst_ref=norm_ea.at[me],
            send_sem=norm_sem.at[2], recv_sem=norm_sem.at[3],
            device_id=device, device_id_type=MESH)

    def copy_norm_sa(t):
        return pltpu.make_async_remote_copy(
            src_ref=norm_own, dst_ref=norm_sa.at[me_sa],
            send_sem=norm_sem.at[0], recv_sem=norm_sem.at[1],
            device_id=partner_sa(t), device_id_type=MESH)

    def all_of(ref, sem):
        return pltpu.make_async_remote_copy(
            src_ref=ref, dst_ref=ref, send_sem=sem, recv_sem=sem,
            device_id=(y, x, pz[1], s0, s1), device_id_type=MESH)

    for block in range(blocks):
        each_partner(lambda other, device, block=block: copy_in(block, other, device).start())

    for n, (rows, step) in enumerate(((count // STEP, STEP), (STEP, 1))):
        row = lax.broadcasted_iota(jnp.int32, (rows, count), 0) * step
        phase = jnp.bitwise_and(row * lax.broadcasted_iota(jnp.int32, (rows, count), 1), count - 1)
        angle = phase.astype(F32) * (2.0 * math.pi / count)
        base[2 * n, :rows] = jnp.cos(angle)
        base[2 * n + 1, :rows] = jnp.sin(angle)

    @pl.loop(0, count // STEP)
    def _(n):
        c_hi, s_hi = base[0, pl.ds(n, 1), :], base[1, pl.ds(n, 1), :]
        c_lo, s_lo = base[2], base[3]
        cosine = (c_hi * c_lo - s_hi * s_lo).astype(BF16)
        sine = (s_hi * c_lo + c_hi * s_lo).astype(BF16)
        rows = pl.ds(pl.multiple_of(n * STEP, STEP), STEP)
        table_a[rows, :count] = cosine
        table_a[rows, count:] = sine
        table_b[rows, :count] = -sine
        table_b[rows, count:] = cosine

    square[...] = jnp.zeros_like(square)
    strip = min(256, count)
    weight = float(count) ** (-1.5)

    def dot(a, b):
        return jnp.dot(a, b, preferred_element_type=F32)

    for block in range(blocks):
        all_of(recv_in.at[block, :, pl.ds(0, peers - 1)], recv_in_sem.at[block]).wait_recv()

        @pl.loop(0, count // strip)
        def _(n, block=block):
            rows = pl.ds(pl.multiple_of(n * strip, strip), strip)
            rows_im = pl.ds(pl.multiple_of(n * strip + count, strip), strip)
            less = recv_in[block, 0:2].reshape(2 * count, columns)
            great = recv_in[block, 2:4].reshape(2 * count, columns)
            less_re, less_im = dot(table_a[rows, :], less), dot(table_b[rows, :], less)
            great_re, great_im = dot(table_a[rows, :], great), dot(table_b[rows, :], great)
            prod[rows, :] = (less_im * great_re - less_re * great_im).astype(BF16)
            prod[rows_im, :] = (less_re * great_re + less_im * great_im).astype(BF16)

        @pl.loop(0, count // strip)
        def _(n, block=block):
            rows = pl.ds(pl.multiple_of(n * strip, strip), strip)
            polar_re = weight * dot(table_a[rows, :], prod[...])
            polar_im = -weight * dot(table_b[rows, :], prod[...])
            for part, value in enumerate((polar_re, polar_im)):
                square[...] += jnp.sum((value * value).reshape(strip // 8, 8, columns), axis=0)
                send_out[block, pl.ds(n * (strip // own), strip // own), part] = value.astype(BF16).reshape(
                    strip // own, own, columns)

        if block == blocks - 1:
            total = jnp.sum(square[...], axis=0, keepdims=True)
            norm_own[...] = functools.reduce(
                jnp.add, [total[:, n * 128:(n + 1) * 128] for n in range(columns // 128)])
            norm_sa[me_sa] = norm_own[...]
            for t in range(1, n0 * n1):
                copy_norm_sa(t).start()
            if n0 * n1 > 1:
                all_of(norm_sa.at[pl.ds(0, n0 * n1 - 1)], norm_sem.at[1]).wait_recv()
            norm_all[...] = functools.reduce(jnp.add, [norm_sa[n] for n in range(n0 * n1)])
            norm_ea[me] = norm_all[...]
            each_partner(lambda other, device: copy_norm(other, device).start())

        recv_out[block, me] = send_out[block, me]
        each_partner(lambda other, device, block=block: copy_out(block, other, device).start())

    for block in range(blocks):
        all_of(recv_out.at[block, pl.ds(0, peers - 1)], recv_out_sem.at[block]).wait_recv()

    all_of(norm_ea.at[pl.ds(0, peers - 1)], norm_sem.at[3]).wait_recv()
    norm = jnp.sum(jnp.sum(norm_ea[...], axis=0), axis=-1, keepdims=True)
    entries = count * blocks * peers * n0 * n1 * columns
    norm_ref[...] = jnp.broadcast_to(jnp.sqrt(norm / entries + 1e-06), norm_ref.shape)

    for block in range(blocks):
        all_of(recv_in.at[block, :, pl.ds(0, peers - 1)], send_sem.at[block]).wait_send()
        all_of(recv_out.at[block, pl.ds(0, peers - 1)], send_sem.at[blocks + block]).wait_send()
    if n0 * n1 > 1:
        all_of(norm_sa.at[pl.ds(0, n0 * n1 - 1)], norm_sem.at[0]).wait_send()
    all_of(norm_ea.at[pl.ds(0, peers - 1)], norm_sem.at[2]).wait_send()


def finish_kernel(recv_ref, out_ref, shuffle, sem):
    blocks, rows, parts, own, columns = recv_ref.shape
    tiles, halves = rows // 8, columns // 128

    for block in range(blocks):
        for part in range(parts):

            @pl.loop(0, tiles)
            def _(tile, block=block, part=part):
                slot = (block * parts + part) * tiles + tile
                for i in range(8):
                    value = recv_ref[block, tile * 8 + i, part].astype(F32)
                    for h in range(halves):
                        shuffle[slot, h, pl.ds(i, own, stride=8), :] = value[:, h * 128:(h + 1) * 128]
                for h in range(halves):
                    pltpu.make_async_copy(
                        shuffle.at[slot, h].reshape(own, 8, 128),
                        out_ref.at[part, :, block, pl.ds(pl.multiple_of(tile * 8, 8), 8), h * 128:(h + 1) * 128],
                        sem).start()

    pltpu.make_async_copy(out_ref, out_ref, sem).wait()


def body(sizes, lesser, greater):
    ny, nx, nz, n0, n1 = sizes
    peers = ny * nx * nz
    own, blocks = 16, 2
    count = own * peers
    columns = lesser.shape[-1]
    vmem = pl.BlockSpec(memory_space=pltpu.VMEM)
    hbm = pl.BlockSpec(memory_space=pltpu.HBM)
    received = (blocks, peers, 2, own, columns)
    raw, norm = pl.pallas_call(
        functools.partial(kernel, sizes),
        out_shape=[jax.ShapeDtypeStruct(received, BF16), jax.ShapeDtypeStruct((1, 128), F32)],
        in_specs=[hbm] * 2,
        out_specs=[vmem, vmem],
        scratch_shapes=[
            pltpu.VMEM((2,) + lesser.shape, BF16),
            pltpu.VMEM((columns // 128, own * 16, 128), F32),
            pltpu.VMEM((blocks, peers, 4, own, columns), BF16),
            pltpu.VMEM((blocks, 4, peers, own, columns), BF16),
            pltpu.VMEM((4, STEP, count), F32),
            pltpu.VMEM((count, 2 * count), BF16),
            pltpu.VMEM((count, 2 * count), BF16),
            pltpu.VMEM((2 * count, columns), BF16),
            pltpu.VMEM(received, BF16),
            pltpu.VMEM((8, columns), F32),
            pltpu.VMEM((1, 128), F32),
            pltpu.VMEM((n0 * n1, 1, 128), F32),
            pltpu.VMEM((peers, 1, 128), F32),
            pltpu.VMEM((1, 128), F32),
            pltpu.SemaphoreType.DMA((2,)),
            pltpu.SemaphoreType.DMA((2 * blocks,)),
            pltpu.SemaphoreType.DMA((blocks,)),
            pltpu.SemaphoreType.DMA((blocks,)),
            pltpu.SemaphoreType.DMA((4,)),
        ],
        compiler_params=pltpu.CompilerParams(
            collective_id=0, has_side_effects=True, vmem_limit_bytes=51 * 1024 * 1024),
        name="polarize",
    )(lesser, greater)
    polar = pl.pallas_call(
        finish_kernel,
        out_shape=jax.ShapeDtypeStruct(lesser.shape, F32),
        in_specs=[vmem],
        out_specs=hbm,
        scratch_shapes=[
            pltpu.VMEM((2 * blocks * (peers // 8), columns // 128, own * 8, 128), F32),
            pltpu.SemaphoreType.DMA,
        ],
        compiler_params=pltpu.CompilerParams(vmem_limit_bytes=16 * 1024 * 1024),
        name="finish",
    )(raw)
    return polar, norm[0, :1]


def solution(mesh):
    sizes = (4, 2, 8, 2, 2)
    finer = Mesh(mesh.devices.reshape(sizes), EA + SA)
    spec = P(None, EA, None, SA, None)
    return jax.shard_map(functools.partial(body, sizes), mesh=finer, in_specs=(spec, spec),
                         out_specs=(spec, P()), check_vma=False)
```
